32 devices in a mesh: tau: 4 (over z), row: 4 (over y, core), col: 2 (over x).
Axes of the slice: x: 2, y: 2, z: 4, core: 2. Of those that a mesh axis runs over, the one named last changes fastest.
Arguments:
- occupied: bfloat16 [4, 1024, 8192], P('tau', 'row', 'col'), may hold values from -6 to 6
- virtual_green: bfloat16 [4, 8192, 2048], P('tau', 'row', 'col'), may hold values from -0.0625 to 0.0625
- occ_mask: int32 [8, 64], P('row', 'col'), may hold values 0 or 1
- virt_mask: int32 [64, 16], P('row', 'col'), may hold values 0 or 1
- chi_mask: int32 [8, 16], P('row', 'col'), may hold values 0 or 1
- cosine_weights: float32 [4, 4], replicated, may hold values from -3 to 3
Outputs:
- chi_freq: float32 [4, 1024, 2048], P(None, ('row', 'tau'), 'col')
The draws below stay inside these ranges and needn't reach their ends.
All inputs are finite; a program needn't handle non-finite values. No bound on the sum of `occ_mask` or of `virt_mask` or of `chi_mask` on one device may be relied on, other than what follows from the above.
Results may differ from the reference program's by a relative error of at most 0.0029.
Values may be sent and summed in bfloat16 or wider, within the bound.
A program may use at most 64 MiB of HBM per device.

```python
import jax
import jax.numpy as jnp
from jax import lax

N = 8192
BLOCK = 128
ROWS = 1024
COLS = 2048
TAU = 4
FREQ = 4


def with_ends(values, rng, smallest, largest):
    longest = values.shape.index(max(values.shape))
    spots = []
    for shift in (0, 1):
        where = [jax.random.randint(jax.random.fold_in(rng, axis), (), 0, length) for axis, length in enumerate(values.shape)]
        where[longest] = (where[longest] + shift) % values.shape[longest]
        spots.append(tuple(where))
    return values.at[spots[0]].set(smallest).at[spots[1]].set(largest)


def shard_levels(stream_key, dims, split, low, high):
    factor_of = 1.0
    for dim, blocks in split:
        steps = jax.random.uniform(jax.random.fold_in(jax.random.fold_in(stream_key, 6), dim), (blocks,), jnp.float32, low / len(split), high / len(split))
        factor_of = factor_of * jnp.repeat(jnp.exp(steps), dims[dim] // blocks).reshape((-1,) + (1,) * (len(dims) - 1 - dim))
    return factor_of


def centred(rng, extent, deviation, most, split=(), kind=jnp.bfloat16):
    factor_of = shard_levels(rng, extent, split, -0.22, 0.18) if split else 1.0
    values = jax.random.normal(rng, extent, jnp.float32) * deviation * factor_of
    return jnp.minimum(jnp.maximum(values, -most), most).astype(kind)


def setup_inputs(seed: int = 0) -> dict:
    seeds = jax.random.split(jax.random.key(seed), 7)
    return {
        "occupied": centred(seeds[0], (TAU, ROWS, N), 1.0, 6.0, ((0, 4), (1, 4), (2, 2))),
        "virtual_green": centred(seeds[1], (TAU, N, COLS), N ** -0.5, 0.0625, ((0, 4), (1, 4), (2, 2))),
        "occ_mask": with_ends((jax.random.randint(seeds[2], (ROWS // BLOCK, N // BLOCK), 0, 4) < 3).astype(jnp.int32), jax.random.fold_in(seeds[2], 1), 0, 1),
        "virt_mask": with_ends((jax.random.randint(seeds[3], (N // BLOCK, COLS // BLOCK), 0, 4) < 3).astype(jnp.int32), jax.random.fold_in(seeds[3], 1), 0, 1),
        "chi_mask": with_ends((jax.random.randint(seeds[4], (ROWS // BLOCK, COLS // BLOCK), 0, 3) < 2).astype(jnp.int32), jax.random.fold_in(seeds[4], 1), 0, 1),
        "cosine_weights": centred(seeds[5], (FREQ, TAU), 0.5, 3.0, (), jnp.float32),
    }


def expand_mask(values, flags):
    block_rows = values.shape[0] // flags.shape[0]
    block_cols = values.shape[1] // flags.shape[1]
    shaped = values.reshape(flags.shape[0], block_rows, flags.shape[1], block_cols)
    masked = shaped * flags.astype(values.dtype)[:, None, :, None]
    return masked.reshape(values.shape)


def reference(occupied, virtual_green, occ_mask, virt_mask, chi_mask, cosine_weights):
    def one_time(pair):
        occ_slab, virt_slab = pair
        product = jnp.dot(expand_mask(occ_slab, occ_mask), expand_mask(virt_slab, virt_mask), preferred_element_type=jnp.float32)
        return expand_mask(product, chi_mask).astype(jnp.bfloat16)

    chi_tau = lax.map(one_time, (occupied, virtual_green))
    return jnp.einsum("kt,tij->kij", cosine_weights.astype(jnp.float32), chi_tau.astype(jnp.float32), precision=lax.Precision.HIGHEST)
```

```python
import functools

import jax
import jax.numpy as jnp
from jax import lax
from jax.experimental import pallas as pl
from jax.experimental.pallas import tpu as pltpu
from jax.sharding import PartitionSpec as P

MESH = pl.DeviceIdType.MESH


def expand_mask(values, flags):
    block_rows = values.shape[0] // flags.shape[0]
    block_cols = values.shape[1] // flags.shape[1]
    shaped = values.reshape(flags.shape[0], block_rows, flags.shape[1], block_cols)
    masked = shaped * flags.astype(values.dtype)[:, None, :, None]
    return masked.reshape(values.shape)


def gathered(occupied, virtual_green, occ_mask, virt_mask, chi_mask, cosine_weights):
    occ_tile = expand_mask(occupied[0], occ_mask)
    virt_tile = expand_mask(virtual_green[0], virt_mask)
    virt_column = lax.all_gather(virt_tile, "row", axis=0, tiled=True)
    accumulated = jnp.dot(
        lax.all_gather(occ_tile, "col", axis=1, tiled=True),
        virt_column,
        preferred_element_type=jnp.float32,
    )
    chi_local = expand_mask(accumulated, chi_mask).astype(jnp.bfloat16)
    regrouped = lax.all_to_all(chi_local[None], "tau", split_axis=1, concat_axis=0, tiled=True)
    return jnp.einsum(
        "kt,tij->kij",
        cosine_weights,
        regrouped.astype(jnp.float32),
        precision=lax.Precision.HIGHEST,
    )


def kernel(
    taus, occ, virt, om, vm, cm, w, out,
    vbuf, vmask, ob, omask, lhs, pa, pbuf, rbuf, cbuf, zbuf,
    v_sem, o_send, o_recv, m_send, m_recv, p_send, p_recv, z_send, z_recv,
):
    tau, row, col = lax.axis_index("tau"), lax.axis_index("row"), lax.axis_index("col")
    half, core = row // 2, row % 2
    diagonal = half == col
    flipped = (1 - half) * 2 + core
    x_peer = {"tau": tau, "row": row, "col": 1 - col}
    y_peer = {"tau": tau, "row": flipped, "col": col}
    far_peer = {"tau": tau, "row": flipped, "col": 1 - col}
    twin = {"tau": tau, "row": half * 2 + 1 - core, "col": col}
    rows = ob.shape[2]
    depth = virt.shape[0]
    block = occ.shape[0] // om.shape[0]
    cols = virt.shape[1]

    def part(step):
        return lax.rem(tau + 1 + step, taus)

    def z_peer(step):
        return {"tau": part(step), "row": row, "col": col}

    def remote(src, dst, send, recv, peer):
        return pltpu.make_async_remote_copy(
            src_ref=src, dst_ref=dst, send_sem=send, recv_sem=recv, device_id=peer, device_id_type=MESH
        )

    mine = pl.ds(pl.multiple_of(core * depth, depth), depth)
    v_local = pltpu.make_async_copy(virt, vbuf.at[mine, :], v_sem.at[0])
    v_local.start()
    vm_rows = vm.shape[0]
    vm_mine = pl.ds(pl.multiple_of(core * vm_rows, vm_rows), vm_rows)
    vm_local = pltpu.make_async_copy(vm, vmask.at[vm_mine, :], v_sem.at[1])
    vm_local.start()

    barrier = pltpu.get_barrier_semaphore()
    peers = [x_peer, y_peer, far_peer, twin] + [z_peer(s) for s in range(taus - 1)]
    for peer in peers:
        pl.semaphore_signal(barrier, inc=1, device_id=peer, device_id_type=MESH)
    pl.semaphore_wait(barrier, len(peers))

    def o_src(step):
        return occ.at[pl.ds(pl.multiple_of(part(step) * rows, rows), rows), :]

    def to_self(src, dst, sem):
        return pltpu.make_async_copy(src, dst, sem)

    def send_part(step):
        src = o_src(step)

        @pl.when(diagonal)
        def _():
            remote(src, ob.at[step, 1], o_send.at[step, 0], o_recv.at[step, 1], x_peer).start()
            to_self(src, ob.at[step, 1], o_recv.at[step, 1]).start()

        @pl.when(jnp.logical_not(diagonal))
        def _():
            remote(src, ob.at[step, 0], o_send.at[step, 1], o_recv.at[step, 0], far_peer).start()
            remote(src, ob.at[step, 0], o_send.at[step, 0], o_recv.at[step, 0], y_peer).start()

    @pl.when(diagonal)
    def _():
        remote(om, omask.at[1], m_send.at[0], m_recv.at[1], x_peer).start()
        to_self(om, omask.at[1], m_recv.at[1]).start()

    @pl.when(jnp.logical_not(diagonal))
    def _():
        remote(om, omask.at[0], m_send.at[1], m_recv.at[0], far_peer).start()
        remote(om, omask.at[0], m_send.at[0], m_recv.at[0], y_peer).start()

    send_part(0)
    v_remote = remote(virt, vbuf.at[mine, :], v_sem.at[2], v_sem.at[3], twin)
    v_remote.start()
    vm_remote = remote(vm, vmask.at[vm_mine, :], v_sem.at[4], v_sem.at[5], twin)
    vm_remote.start()
    if taus > 1:
        send_part(1)

    deep = depth // vm_rows

    def mask_virt(base):
        def one(b, _):
            r = pl.ds(pl.multiple_of((base + b) * deep, deep), deep)
            flags = vmask[pl.ds(base + b, 1), :]
            vbuf[r, :] = vbuf[r, :] * jnp.broadcast_to(flags, (deep, cols)).astype(vbuf.dtype)
            return 0

        lax.fori_loop(0, vm_rows, one, 0)

    v_local.wait()
    vm_local.wait()
    mask_virt(core * vm_rows)
    v_remote.wait_recv()
    vm_remote.wait_recv()
    mask_virt((1 - core) * vm_rows)
    for slot in range(2):
        to_self(om, omask.at[slot], m_recv.at[slot]).wait()

    tile = 256

    def partial_copy(step):
        return remote(pbuf.at[step], rbuf.at[step], p_send.at[step], p_recv.at[step], y_peer)

    def z_copy(step):
        return remote(cbuf.at[step], zbuf.at[tau], z_send.at[step], z_recv.at[step], z_peer(step))

    def flag_row(step):
        return part(step) * rows // block

    def finish(step):
        partial_copy(step).wait_recv()
        flags = jnp.broadcast_to(cm[pl.ds(flag_row(step), 1), :], (rows, cols))
        chi = ((pa[step] + rbuf[step].astype(jnp.float32)) * flags).astype(jnp.bfloat16)
        if step < taus - 1:
            cbuf[step] = chi
            z_copy(step).start()
        else:
            zbuf[tau] = chi

    for step in range(taus):
        for slot in range(2):
            to_self(o_src(step), ob.at[step, slot], o_recv.at[step, slot]).wait()
            flags = omask[slot, pl.ds(flag_row(step), 1), :]
            lhs[pl.ds(slot * rows, rows), :] = ob[step, slot] * jnp.broadcast_to(
                flags, (rows, lhs.shape[1])
            ).astype(lhs.dtype)

        def one(n, _, step=step):
            c = pl.ds(pl.multiple_of(n * tile, tile), tile)
            r = jnp.dot(lhs[...], vbuf[:, c], preferred_element_type=jnp.float32)
            pbuf[step, :, c] = r[:rows].astype(jnp.bfloat16)
            pa[step, :, c] = r[rows:]
            return 0

        lax.fori_loop(0, cols // tile, one, 0)
        partial_copy(step).start()
        if step + 2 < taus:
            send_part(step + 2)
        if step > 0:
            finish(step - 1)
    finish(taus - 1)

    for step in range(taus - 1):
        z_copy(step).wait_recv()
    for k in range(out.shape[0]):
        total = w[k, 0] * zbuf[0].astype(jnp.float32)
        for t in range(1, taus):
            total = total + w[k, t] * zbuf[t].astype(jnp.float32)
        out[k] = total

    for step in range(taus - 1):
        z_copy(step).wait_send()
    for step in range(taus):
        partial_copy(step).wait_send()
        remote(o_src(step), ob.at[step, 1], o_send.at[step, 0], o_recv.at[step, 1], x_peer).wait_send()
    remote(om, omask.at[1], m_send.at[0], m_recv.at[1], x_peer).wait_send()

    @pl.when(jnp.logical_not(diagonal))
    def _():
        for step in range(taus):
            remote(o_src(step), ob.at[step, 0], o_send.at[step, 1], o_recv.at[step, 0], far_peer).wait_send()
        remote(om, omask.at[0], m_send.at[1], m_recv.at[0], far_peer).wait_send()

    v_remote.wait_send()
    vm_remote.wait_send()


def exchanged(taus, occupied, virtual_green, occ_mask, virt_mask, chi_mask, cosine_weights):
    occ, virt = occupied[0], virtual_green[0]
    m, k = occ.shape
    depth, cols = virt.shape
    rows = m // taus
    om = jnp.repeat(occ_mask.astype(jnp.float32), k // occ_mask.shape[1], axis=1)
    vm = jnp.repeat(virt_mask.astype(jnp.float32), cols // virt_mask.shape[1], axis=1)
    cm = jnp.repeat(chi_mask.astype(jnp.float32), cols // chi_mask.shape[1], axis=1)
    bf16, f32 = jnp.bfloat16, jnp.float32
    dma = pltpu.SemaphoreType.DMA
    vmem = pl.BlockSpec(memory_space=pltpu.VMEM)
    return pl.pallas_call(
        functools.partial(kernel, taus),
        out_shape=jax.ShapeDtypeStruct((cosine_weights.shape[0], rows, cols), f32),
        in_specs=[
            pl.BlockSpec(memory_space=pl.ANY),
            pl.BlockSpec(memory_space=pl.ANY),
            vmem,
            vmem,
            vmem,
            pl.BlockSpec(memory_space=pltpu.SMEM),
        ],
        out_specs=vmem,
        scratch_shapes=[
            pltpu.VMEM((2 * depth, cols), bf16),
            pltpu.VMEM((2 * vm.shape[0], cols), f32),
            pltpu.VMEM((taus, 2, rows, k), bf16),
            pltpu.VMEM((2,) + om.shape, f32),
            pltpu.VMEM((2 * rows, k), bf16),
            pltpu.VMEM((taus, rows, cols), f32),
            pltpu.VMEM((taus, rows, cols), bf16),
            pltpu.VMEM((taus, rows, cols), bf16),
            pltpu.VMEM((taus, rows, cols), bf16),
            pltpu.VMEM((taus, rows, cols), bf16),
            dma((6,)),
            dma((taus, 2)),
            dma((taus, 2)),
            dma((2,)),
            dma((2,)),
            dma((taus,)),
            dma((taus,)),
            dma((taus,)),
            dma((taus,)),
        ],
        compiler_params=pltpu.CompilerParams(collective_id=0, has_side_effects=True),
    )(occ, virt, om, vm, cm, cosine_weights)


def solution(mesh):
    placed = (
        P("tau", "row", "col"),
        P("tau", "row", "col"),
        P("row", "col"),
        P("row", "col"),
        P("row", "col"),
        P(),
    )
    plane = mesh.shape["row"] == 4 and mesh.shape["col"] == 2
    return jax.shard_map(
        functools.partial(exchanged, mesh.shape["tau"]) if plane else gathered,
        mesh=mesh,
        in_specs=placed,
        out_specs=P(None, ("row", "tau"), "col"),
        check_vma=False,
    )
```

```python
import functools

import jax
import jax.numpy as jnp
from jax import lax
from jax.experimental import pallas as pl
from jax.experimental.pallas import tpu as pltpu
from jax.sharding import PartitionSpec as P

MESH = pl.DeviceIdType.MESH


def expand_mask(values, flags):
    block_rows = values.shape[0] // flags.shape[0]
    block_cols = values.shape[1] // flags.shape[1]
    shaped = values.reshape(flags.shape[0], block_rows, flags.shape[1], block_cols)
    masked = shaped * flags.astype(values.dtype)[:, None, :, None]
    return masked.reshape(values.shape)


def gathered(occupied, virtual_green, occ_mask, virt_mask, chi_mask, cosine_weights):
    occ_tile = expand_mask(occupied[0], occ_mask)
    virt_tile = expand_mask(virtual_green[0], virt_mask)
    virt_column = lax.all_gather(virt_tile, "row", axis=0, tiled=True)
    accumulated = jnp.dot(
        lax.all_gather(occ_tile, "col", axis=1, tiled=True),
        virt_column,
        preferred_element_type=jnp.float32,
    )
    chi_local = expand_mask(accumulated, chi_mask).astype(jnp.bfloat16)
    regrouped = lax.all_to_all(chi_local[None], "tau", split_axis=1, concat_axis=0, tiled=True)
    return jnp.einsum(
        "kt,tij->kij",
        cosine_weights,
        regrouped.astype(jnp.float32),
        precision=lax.Precision.HIGHEST,
    )


def spread(flags, width, transposed=False):
    dim = 0 if transposed else 1
    count = flags.shape[dim]
    owner = lax.broadcasted_iota(jnp.int32, (count, count * width), 1) // width
    mine = owner == lax.broadcasted_iota(jnp.int32, (count, count * width), 0)
    return lax.dot_general(
        flags.astype(jnp.float32),
        mine.astype(jnp.float32),
        (((dim,), (0,)), ((), ())),
        preferred_element_type=jnp.float32,
    )


def kernel(
    taus, occ, virt, om, vm, cm, zbuf,
    vbuf, vraw, vmask, ob, oraw, omask, cmask, lhs, pa, pbuf, rbuf, cbuf,
    v_sem, o_send, o_recv, f_send, m_send, m_recv, p_send, p_recv, z_send, z_recv,
):
    tau, row, col = lax.axis_index("tau"), lax.axis_index("row"), lax.axis_index("col")
    half, core = row // 2, row % 2
    diagonal = half == col
    flipped = (1 - half) * 2 + core
    x_peer = {"tau": tau, "row": row, "col": 1 - col}
    y_peer = {"tau": tau, "row": flipped, "col": col}
    far_peer = {"tau": tau, "row": flipped, "col": 1 - col}
    twin = {"tau": tau, "row": half * 2 + 1 - core, "col": col}
    steps = 2 * taus
    rows = ob.shape[2]
    depth = virt.shape[0]
    block = occ.shape[0] // om.shape[0]
    cols = virt.shape[1]
    near_only, far_only = 2, 3

    def start_row(step):
        return lax.rem(tau + 1 + step // 2, taus) * (2 * rows) + (step % 2) * rows

    def z_peer(step):
        return {"tau": lax.rem(tau + 1 + step // 2, taus), "row": row, "col": col}

    def remote(src, dst, send, recv, peer):
        return pltpu.make_async_remote_copy(
            src_ref=src, dst_ref=dst, send_sem=send, recv_sem=recv, device_id=peer, device_id_type=MESH
        )

    mine = pl.ds(pl.multiple_of(core * depth, depth), depth)
    v_local = pltpu.make_async_copy(virt, vbuf.at[mine, :], v_sem.at[0])
    v_local.start()

    barrier = pltpu.get_barrier_semaphore()
    peers = [x_peer, y_peer, far_peer, twin] + [z_peer(2 * s) for s in range(taus - 1)]
    for peer in peers:
        pl.semaphore_signal(barrier, inc=1, device_id=peer, device_id_type=MESH)
    pl.semaphore_wait(barrier, len(peers))

    def o_src(step):
        return occ.at[pl.ds(pl.multiple_of(start_row(step), rows), rows), :]

    def on_diagonal(step):
        return remote(o_src(step), ob.at[step, 1], o_send.at[step, 0], o_recv.at[step, 1], x_peer)

    def own(step):
        return pltpu.make_async_copy(o_src(step), ob.at[step, 1], o_recv.at[step, 1])

    def near(step):
        return remote(o_src(step), ob.at[step, 0], o_send.at[step, 0], o_recv.at[step, 0], y_peer)

    def far(step):
        return remote(o_src(step), ob.at[step, 0], o_send.at[step, 1], o_recv.at[step, 0], far_peer)

    def forward(step):
        return remote(ob.at[step, 0], ob.at[step, 0], f_send.at[0], o_recv.at[step, 0], x_peer)

    def arrived(step, slot):
        return pltpu.make_async_copy(o_src(step), ob.at[step, slot], o_recv.at[step, slot])

    m_x = remote(om, oraw.at[1], m_send.at[0], m_recv.at[1], x_peer)
    m_own = pltpu.make_async_copy(om, oraw.at[1], m_recv.at[1])
    m_near = remote(om, oraw.at[0], m_send.at[0], m_recv.at[0], y_peer)
    m_far = remote(om, oraw.at[0], m_send.at[1], m_recv.at[0], far_peer)
    v_remote = remote(virt, vbuf.at[mine, :], v_sem.at[1], v_sem.at[2], twin)
    vm_remote = remote(vm, vraw, v_sem.at[3], v_sem.at[4], twin)

    @pl.when(diagonal)
    def _():
        m_x.start()
        m_own.start()
        for step in (0, 1, 2):
            on_diagonal(step).start()
            own(step).start()

    @pl.when(jnp.logical_not(diagonal))
    def _():
        m_far.start()
        m_near.start()
        far(0).start()
        near(0).start()
        far(far_only).start()
        near(near_only).start()
        far(1).start()
        near(1).start()

    vm_remote.start()
    v_remote.start()

    vm_rows = vm.shape[1]
    deep = depth // vm_rows

    def mask_virt(base):
        def one(b, _):
            r = pl.ds(pl.multiple_of((base + b) * deep, deep), deep)
            flags = vmask[pl.ds(base + b, 1), :]
            vbuf[r, :] = vbuf[r, :] * jnp.broadcast_to(flags, (deep, cols)).astype(vbuf.dtype)
            return 0

        lax.fori_loop(0, vm_rows, one, 0)

    width = cols // vm.shape[0]
    vmask[pl.ds(pl.multiple_of(core * vm_rows, vm_rows), vm_rows), :] = spread(vm[...], width, True)
    cmask[...] = spread(cm[...], cols // cm.shape[1])
    vm_remote.wait_recv()
    vmask[pl.ds(pl.multiple_of((1 - core) * vm_rows, vm_rows), vm_rows), :] = spread(vraw[...], width, True)
    v_local.wait()
    mask_virt(core * vm_rows)
    for slot in range(2):
        pltpu.make_async_copy(om, oraw.at[slot], m_recv.at[slot]).wait()
        omask[slot] = spread(oraw[slot], occ.shape[1] // om.shape[1])
    v_remote.wait_recv()
    mask_virt((1 - core) * vm_rows)

    tile = 256

    def partial_copy(step):
        return remote(pbuf.at[step], rbuf.at[step], p_send.at[step], p_recv.at[step], y_peer)

    def z_copy(step):
        dst = zbuf.at[tau, pl.ds((step % 2) * rows, rows), :]
        return remote(cbuf.at[step], dst, z_send.at[step], z_recv.at[step], z_peer(step))

    def flag_row(step):
        return start_row(step) // block

    def finish(step):
        partial_copy(step).wait_recv()
        flags = jnp.broadcast_to(cmask[pl.ds(flag_row(step), 1), :], (rows, cols))
        chi = ((pa[step % 2] + rbuf[step].astype(jnp.float32)) * flags).astype(jnp.bfloat16)
        if step < steps - 2:
            cbuf[step] = chi
            z_copy(step).start()
        else:
            zbuf[tau, pl.ds((step % 2) * rows, rows), :] = chi

    for step in range(steps):
        for slot in range(2):
            if not (slot == 0 and step in (near_only, far_only)):
                arrived(step, slot).wait()
            elif step == near_only:
                @pl.when(jnp.logical_not(diagonal))
                def _():
                    arrived(near_only, 0).wait()
            else:
                @pl.when(diagonal)
                def _():
                    arrived(far_only, 0).wait()
            flags = omask[slot, pl.ds(flag_row(step), 1), :]
            lhs[pl.ds(slot * rows, rows), :] = ob[step, slot] * jnp.broadcast_to(
                flags, (rows, lhs.shape[1])
            ).astype(lhs.dtype)

        def one(n, _, step=step):
            c = pl.ds(pl.multiple_of(n * tile, tile), tile)
            r = jnp.dot(lhs[...], vbuf[:, c], preferred_element_type=jnp.float32)
            pbuf[step, :, c] = r[:rows].astype(jnp.bfloat16)
            pa[step % 2, :, c] = r[rows:]
            return 0

        lax.fori_loop(0, cols // tile, one, 0)
        partial_copy(step).start()

        @pl.when(diagonal)
        def _(step=step):
            if step == 0:
                arrived(near_only, 0).wait()
                forward(near_only).start()
            for later in ((3, 4) if step == 0 else (step + 4,)):
                if later < steps:
                    on_diagonal(later).start()
                    own(later).start()

        @pl.when(jnp.logical_not(diagonal))
        def _(step=step):
            if step == 0:
                arrived(far_only, 0).wait()
                forward(far_only).start()
            if step + 4 < steps:
                far(step + 4).start()
                near(step + 4).start()

        if step > 0:
            finish(step - 1)
    finish(steps - 1)

    for step in range(steps - 2):
        z_copy(step).wait_recv()
    for step in range(steps - 2):
        z_copy(step).wait_send()
    for step in range(steps):
        partial_copy(step).wait_send()

    @pl.when(diagonal)
    def _():
        for step in range(steps):
            on_diagonal(step).wait_send()
        forward(near_only).wait_send()
        m_x.wait_send()

    @pl.when(jnp.logical_not(diagonal))
    def _():
        for step in range(steps):
            if step != near_only:
                far(step).wait_send()
            if step != far_only:
                near(step).wait_send()
        forward(far_only).wait_send()
        m_far.wait_send()
        m_near.wait_send()

    v_remote.wait_send()
    vm_remote.wait_send()


def transform(w, z, out):
    points = [z[t].astype(jnp.float32) for t in range(z.shape[0])]
    for k in range(out.shape[0]):
        total = w[k, 0] * points[0]
        for t in range(1, len(points)):
            total = total + w[k, t] * points[t]
        out[k] = total


def exchanged(taus, occupied, virtual_green, occ_mask, virt_mask, chi_mask, cosine_weights):
    occ, virt = occupied[0], virtual_green[0]
    m, k = occ.shape
    depth, cols = virt.shape
    rows = m // (2 * taus)
    steps = 2 * taus
    bf16, f32, i32 = jnp.bfloat16, jnp.float32, jnp.int32
    dma = pltpu.SemaphoreType.DMA
    vmem = pl.BlockSpec(memory_space=pltpu.VMEM)
    vm = virt_mask.T
    points = pl.pallas_call(
        functools.partial(kernel, taus),
        out_shape=jax.ShapeDtypeStruct((taus, 2 * rows, cols), bf16),
        in_specs=[pl.BlockSpec(memory_space=pl.ANY), pl.BlockSpec(memory_space=pl.ANY), vmem, vmem, vmem],
        out_specs=vmem,
        scratch_shapes=[
            pltpu.VMEM((2 * depth, cols), bf16),
            pltpu.VMEM(vm.shape, i32),
            pltpu.VMEM((2 * vm.shape[1], cols), f32),
            pltpu.VMEM((steps, 2, rows, k), bf16),
            pltpu.VMEM((2,) + occ_mask.shape, i32),
            pltpu.VMEM((2, occ_mask.shape[0], k), f32),
            pltpu.VMEM((chi_mask.shape[0], cols), f32),
            pltpu.VMEM((2 * rows, k), bf16),
            pltpu.VMEM((2, rows, cols), f32),
            pltpu.VMEM((steps, rows, cols), bf16),
            pltpu.VMEM((steps, rows, cols), bf16),
            pltpu.VMEM((steps, rows, cols), bf16),
            dma((5,)),
            dma((steps, 2)),
            dma((steps, 2)),
            dma((1,)),
            dma((2,)),
            dma((2,)),
            dma((steps,)),
            dma((steps,)),
            dma((steps,)),
            dma((steps,)),
        ],
        compiler_params=pltpu.CompilerParams(collective_id=0, has_side_effects=True),
    )(occ, virt, occ_mask, vm, chi_mask)
    freqs = cosine_weights.shape[0]
    return pl.pallas_call(
        transform,
        grid=(2,),
        out_shape=jax.ShapeDtypeStruct((freqs, 2 * rows, cols), f32),
        in_specs=[
            pl.BlockSpec(memory_space=pltpu.SMEM),
            pl.BlockSpec((taus, rows, cols), lambda i: (0, i, 0)),
        ],
        out_specs=pl.BlockSpec((freqs, rows, cols), lambda i: (0, i, 0)),
    )(cosine_weights, points)


def solution(mesh):
    placed = (
        P("tau", "row", "col"),
        P("tau", "row", "col"),
        P("row", "col"),
        P("row", "col"),
        P("row", "col"),
        P(),
    )
    plane = mesh.shape["row"] == 4 and mesh.shape["col"] == 2 and mesh.shape["tau"] > 1
    return jax.shard_map(
        functools.partial(exchanged, mesh.shape["tau"]) if plane else gathered,
        mesh=mesh,
        in_specs=placed,
        out_specs=P(None, ("row", "tau"), "col"),
        check_vma=False,
    )
```

```python
import functools

import jax
import jax.numpy as jnp
from jax import lax
from jax.experimental import pallas as pl
from jax.experimental.pallas import tpu as pltpu
from jax.sharding import PartitionSpec as P

MESH = pl.DeviceIdType.MESH


def expand_mask(values, flags):
    block_rows = values.shape[0] // flags.shape[0]
    block_cols = values.shape[1] // flags.shape[1]
    shaped = values.reshape(flags.shape[0], block_rows, flags.shape[1], block_cols)
    masked = shaped * flags.astype(values.dtype)[:, None, :, None]
    return masked.reshape(values.shape)


def gathered(occupied, virtual_green, occ_mask, virt_mask, chi_mask, cosine_weights):
    occ_tile = expand_mask(occupied[0], occ_mask)
    virt_tile = expand_mask(virtual_green[0], virt_mask)
    virt_column = lax.all_gather(virt_tile, "row", axis=0, tiled=True)
    accumulated = jnp.dot(
        lax.all_gather(occ_tile, "col", axis=1, tiled=True),
        virt_column,
        preferred_element_type=jnp.float32,
    )
    chi_local = expand_mask(accumulated, chi_mask).astype(jnp.bfloat16)
    regrouped = lax.all_to_all(chi_local[None], "tau", split_axis=1, concat_axis=0, tiled=True)
    return jnp.einsum(
        "kt,tij->kij",
        cosine_weights,
        regrouped.astype(jnp.float32),
        precision=lax.Precision.HIGHEST,
    )


def spread(flags, width, transposed=False):
    dim = 0 if transposed else 1
    count = flags.shape[dim]
    owner = lax.broadcasted_iota(jnp.int32, (count, count * width), 1) // width
    mine = owner == lax.broadcasted_iota(jnp.int32, (count, count * width), 0)
    return lax.dot_general(
        flags.astype(jnp.float32),
        mine.astype(jnp.float32),
        (((dim,), (0,)), ((), ())),
        preferred_element_type=jnp.float32,
    )


def kernel(
    taus, occ, virt, om, vm, cm, zbuf,
    vbuf, vraw, vmask, ob, oraw, omask, cmask, lhs, pa, pbuf, rbuf, cbuf,
    v_sem, o_send, o_recv, f_send, m_send, m_recv, p_send, p_recv, z_send, z_recv,
):
    tau, row, col = lax.axis_index("tau"), lax.axis_index("row"), lax.axis_index("col")
    half, core = row // 2, row % 2
    diagonal = half == col
    flipped = (1 - half) * 2 + core
    x_peer = {"tau": tau, "row": row, "col": 1 - col}
    y_peer = {"tau": tau, "row": flipped, "col": col}
    far_peer = {"tau": tau, "row": flipped, "col": 1 - col}
    twin = {"tau": tau, "row": half * 2 + 1 - core, "col": col}
    steps = 2 * taus
    rows = ob.shape[2]
    depth = virt.shape[0]
    block = occ.shape[0] // om.shape[0]
    cols = virt.shape[1]
    near_only, far_only = 2, 3

    def start_row(step):
        return lax.rem(tau + 1 + step // 2, taus) * (2 * rows) + (step % 2) * rows

    def z_peer(step):
        return {"tau": lax.rem(tau + 1 + step // 2, taus), "row": row, "col": col}

    def remote(src, dst, send, recv, peer):
        return pltpu.make_async_remote_copy(
            src_ref=src, dst_ref=dst, send_sem=send, recv_sem=recv, device_id=peer, device_id_type=MESH
        )

    mine = pl.ds(pl.multiple_of(core * depth, depth), depth)
    v_local = pltpu.make_async_copy(virt, vbuf.at[mine, :], v_sem.at[0])
    v_local.start()

    barrier = pltpu.get_barrier_semaphore()
    peers = [x_peer, y_peer, far_peer, twin] + [z_peer(2 * s) for s in range(taus - 1)]
    for peer in peers:
        pl.semaphore_signal(barrier, inc=1, device_id=peer, device_id_type=MESH)
    pl.semaphore_wait(barrier, len(peers))

    def o_src(step):
        return occ.at[pl.ds(pl.multiple_of(start_row(step), rows), rows), :]

    def on_diagonal(step):
        return remote(o_src(step), ob.at[step, 1], o_send.at[step, 0], o_recv.at[step, 1], x_peer)

    def own(step):
        return pltpu.make_async_copy(o_src(step), ob.at[step, 1], o_recv.at[step, 1])

    def near(step):
        return remote(o_src(step), ob.at[step, 0], o_send.at[step, 0], o_recv.at[step, 0], y_peer)

    def far(step):
        return remote(o_src(step), ob.at[step, 0], o_send.at[step, 1], o_recv.at[step, 0], far_peer)

    def forward(step):
        return remote(ob.at[step, 0], ob.at[step, 0], f_send.at[0], o_recv.at[step, 0], x_peer)

    def arrived(step, slot):
        return pltpu.make_async_copy(o_src(step), ob.at[step, slot], o_recv.at[step, slot])

    m_x = remote(om, oraw.at[1], m_send.at[0], m_recv.at[1], x_peer)
    m_own = pltpu.make_async_copy(om, oraw.at[1], m_recv.at[1])
    m_near = remote(om, oraw.at[0], m_send.at[0], m_recv.at[0], y_peer)
    m_far = remote(om, oraw.at[0], m_send.at[1], m_recv.at[0], far_peer)
    v_remote = remote(virt, vbuf.at[mine, :], v_sem.at[1], v_sem.at[2], twin)
    vm_remote = remote(vm, vraw, v_sem.at[3], v_sem.at[4], twin)

    @pl.when(diagonal)
    def _():
        m_x.start()
        m_own.start()
        for step in (0, 1, 2):
            on_diagonal(step).start()
            own(step).start()

    @pl.when(jnp.logical_not(diagonal))
    def _():
        m_far.start()
        m_near.start()
        far(0).start()
        near(0).start()
        far(far_only).start()
        near(near_only).start()
        far(1).start()
        near(1).start()

    vm_remote.start()
    v_remote.start()

    vm_rows = vm.shape[1]
    deep = depth // vm_rows

    def mask_virt(base):
        def one(b, _):
            r = pl.ds(pl.multiple_of((base + b) * deep, deep), deep)
            flags = vmask[pl.ds(base + b, 1), :]
            vbuf[r, :] = vbuf[r, :] * jnp.broadcast_to(flags, (deep, cols)).astype(vbuf.dtype)
            return 0

        lax.fori_loop(0, vm_rows, one, 0)

    width = cols // vm.shape[0]
    vmask[pl.ds(pl.multiple_of(core * vm_rows, vm_rows), vm_rows), :] = spread(vm[...], width, True)
    cmask[...] = spread(cm[...], cols // cm.shape[1])
    vm_remote.wait_recv()
    vmask[pl.ds(pl.multiple_of((1 - core) * vm_rows, vm_rows), vm_rows), :] = spread(vraw[...], width, True)
    v_local.wait()
    mask_virt(core * vm_rows)
    for slot in range(2):
        pltpu.make_async_copy(om, oraw.at[slot], m_recv.at[slot]).wait()
        omask[slot] = spread(oraw[slot], occ.shape[1] // om.shape[1])
    v_remote.wait_recv()
    mask_virt((1 - core) * vm_rows)

    tile = 256

    def partial_copy(step):
        return remote(pbuf.at[step], rbuf.at[step], p_send.at[step], p_recv.at[step], y_peer)

    def z_copy(step):
        dst = zbuf.at[tau, pl.ds((step % 2) * rows, rows), :]
        return remote(cbuf.at[step], dst, z_send.at[step], z_recv.at[step], z_peer(step))

    def flag_row(step):
        return start_row(step) // block

    def finish(step):
        partial_copy(step).wait_recv()
        flags = jnp.broadcast_to(cmask[pl.ds(flag_row(step), 1), :], (rows, cols))
        chi = ((pa[step % 2] + rbuf[step].astype(jnp.float32)) * flags).astype(jnp.bfloat16)
        if step < steps - 2:
            cbuf[step] = chi
            z_copy(step).start()
        else:
            zbuf[tau, pl.ds((step % 2) * rows, rows), :] = chi

    def load(step, slot):
        def wait():
            arrived(step, slot).wait()

        if slot == 0 and step == near_only:
            pl.when(jnp.logical_not(diagonal))(wait)
        elif slot == 0 and step == far_only:
            pl.when(diagonal)(wait)
        else:
            wait()
        flags = omask[slot, pl.ds(flag_row(step), 1), :]
        lhs[pl.ds(slot * rows, rows), :] = ob[step, slot] * jnp.broadcast_to(
            flags, (rows, lhs.shape[1])
        ).astype(lhs.dtype)

    for step in range(-1, steps):
        ahead = step + 1
        first, last = step < 0, ahead == steps
        if not last:
            load(ahead, 0)
        if not first:
            load(step, 1)

        def one(n, _, step=step, ahead=ahead, first=first, last=last):
            c = pl.ds(pl.multiple_of(n * tile, tile), tile)
            base, end = (rows if last else 0), (rows if first else 2 * rows)
            r = jnp.dot(lhs[base:end, :], vbuf[:, c], preferred_element_type=jnp.float32)
            if not last:
                pbuf[ahead, :, c] = r[:rows].astype(jnp.bfloat16)
            if not first:
                pa[step % 2, :, c] = r[rows - base :]
            return 0

        lax.fori_loop(0, cols // tile, one, 0)
        if not last:
            partial_copy(ahead).start()

        @pl.when(diagonal)
        def _(ahead=ahead, first=first):
            if first:
                arrived(near_only, 0).wait()
                forward(near_only).start()
            for later in ((3, 4) if first else (ahead + 4,)):
                if later < steps:
                    on_diagonal(later).start()
                    own(later).start()

        @pl.when(jnp.logical_not(diagonal))
        def _(ahead=ahead, first=first):
            if first:
                arrived(far_only, 0).wait()
                forward(far_only).start()
            if ahead + 4 < steps:
                far(ahead + 4).start()
                near(ahead + 4).start()

        if not first:
            finish(step)

    for step in range(steps - 2):
        z_copy(step).wait_recv()
    for step in range(steps - 2):
        z_copy(step).wait_send()
    for step in range(steps):
        partial_copy(step).wait_send()

    @pl.when(diagonal)
    def _():
        for step in range(steps):
            on_diagonal(step).wait_send()
        forward(near_only).wait_send()
        m_x.wait_send()

    @pl.when(jnp.logical_not(diagonal))
    def _():
        for step in range(steps):
            if step != near_only:
                far(step).wait_send()
            if step != far_only:
                near(step).wait_send()
        forward(far_only).wait_send()
        m_far.wait_send()
        m_near.wait_send()

    v_remote.wait_send()
    vm_remote.wait_send()


def transform(w, z, out):
    points = [z[t].astype(jnp.float32) for t in range(z.shape[0])]
    for k in range(out.shape[0]):
        total = w[k, 0] * points[0]
        for t in range(1, len(points)):
            total = total + w[k, t] * points[t]
        out[k] = total


def exchanged(taus, occupied, virtual_green, occ_mask, virt_mask, chi_mask, cosine_weights):
    occ, virt = occupied[0], virtual_green[0]
    m, k = occ.shape
    depth, cols = virt.shape
    rows = m // (2 * taus)
    steps = 2 * taus
    bf16, f32, i32 = jnp.bfloat16, jnp.float32, jnp.int32
    dma = pltpu.SemaphoreType.DMA
    vmem = pl.BlockSpec(memory_space=pltpu.VMEM)
    vm = virt_mask.T
    points = pl.pallas_call(
        functools.partial(kernel, taus),
        out_shape=jax.ShapeDtypeStruct((taus, 2 * rows, cols), bf16),
        in_specs=[pl.BlockSpec(memory_space=pl.ANY), pl.BlockSpec(memory_space=pl.ANY), vmem, vmem, vmem],
        out_specs=vmem,
        scratch_shapes=[
            pltpu.VMEM((2 * depth, cols), bf16),
            pltpu.VMEM(vm.shape, i32),
            pltpu.VMEM((2 * vm.shape[1], cols), f32),
            pltpu.VMEM((steps, 2, rows, k), bf16),
            pltpu.VMEM((2,) + occ_mask.shape, i32),
            pltpu.VMEM((2, occ_mask.shape[0], k), f32),
            pltpu.VMEM((chi_mask.shape[0], cols), f32),
            pltpu.VMEM((2 * rows, k), bf16),
            pltpu.VMEM((2, rows, cols), f32),
            pltpu.VMEM((steps, rows, cols), bf16),
            pltpu.VMEM((steps, rows, cols), bf16),
            pltpu.VMEM((steps, rows, cols), bf16),
            dma((5,)),
            dma((steps, 2)),
            dma((steps, 2)),
            dma((1,)),
            dma((2,)),
            dma((2,)),
            dma((steps,)),
            dma((steps,)),
            dma((steps,)),
            dma((steps,)),
        ],
        compiler_params=pltpu.CompilerParams(collective_id=0, has_side_effects=True),
    )(occ, virt, occ_mask, vm, chi_mask)
    freqs = cosine_weights.shape[0]
    return pl.pallas_call(
        transform,
        grid=(2,),
        out_shape=jax.ShapeDtypeStruct((freqs, 2 * rows, cols), f32),
        in_specs=[
            pl.BlockSpec(memory_space=pltpu.SMEM),
            pl.BlockSpec((taus, rows, cols), lambda i: (0, i, 0)),
        ],
        out_specs=pl.BlockSpec((freqs, rows, cols), lambda i: (0, i, 0)),
    )(cosine_weights, points)


def solution(mesh):
    placed = (
        P("tau", "row", "col"),
        P("tau", "row", "col"),
        P("row", "col"),
        P("row", "col"),
        P("row", "col"),
        P(),
    )
    plane = mesh.shape["row"] == 4 and mesh.shape["col"] == 2 and mesh.shape["tau"] > 1
    return jax.shard_map(
        functools.partial(exchanged, mesh.shape["tau"]) if plane else gathered,
        mesh=mesh,
        in_specs=placed,
        out_specs=P(None, ("row", "tau"), "col"),
        check_vma=False,
    )
```

```python
import functools

import jax
import jax.numpy as jnp
from jax import lax
from jax.experimental import pallas as pl
from jax.experimental.pallas import tpu as pltpu
from jax.sharding import PartitionSpec as P

MESH = pl.DeviceIdType.MESH


def expand_mask(values, flags):
    block_rows = values.shape[0] // flags.shape[0]
    block_cols = values.shape[1] // flags.shape[1]
    shaped = values.reshape(flags.shape[0], block_rows, flags.shape[1], block_cols)
    masked = shaped * flags.astype(values.dtype)[:, None, :, None]
    return masked.reshape(values.shape)


def gathered(occupied, virtual_green, occ_mask, virt_mask, chi_mask, cosine_weights):
    occ_tile = expand_mask(occupied[0], occ_mask)
    virt_tile = expand_mask(virtual_green[0], virt_mask)
    virt_column = lax.all_gather(virt_tile, "row", axis=0, tiled=True)
    accumulated = jnp.dot(
        lax.all_gather(occ_tile, "col", axis=1, tiled=True),
        virt_column,
        preferred_element_type=jnp.float32,
    )
    chi_local = expand_mask(accumulated, chi_mask).astype(jnp.bfloat16)
    regrouped = lax.all_to_all(chi_local[None], "tau", split_axis=1, concat_axis=0, tiled=True)
    return jnp.einsum(
        "kt,tij->kij",
        cosine_weights,
        regrouped.astype(jnp.float32),
        precision=lax.Precision.HIGHEST,
    )


def spread(flags, width, transposed=False):
    dim = 0 if transposed else 1
    count = flags.shape[dim]
    owner = lax.broadcasted_iota(jnp.int32, (count, count * width), 1) // width
    mine = owner == lax.broadcasted_iota(jnp.int32, (count, count * width), 0)
    return lax.dot_general(
        flags.astype(jnp.float32),
        mine.astype(jnp.float32),
        (((dim,), (0,)), ((), ())),
        preferred_element_type=jnp.float32,
    )


def kernel(
    taus, occ, virt, om, vm, cm, zbuf,
    vbuf, vraw, vmask, ob, oraw, omask, cmask, lhs, pa, pbuf, rbuf, cbuf,
    v_sem, o_send, o_recv, h_recv, f_send, m_send, m_recv, p_send, p_recv, z_send, z_recv,
):
    tau, row, col = lax.axis_index("tau"), lax.axis_index("row"), lax.axis_index("col")
    half, core = row // 2, row % 2
    diagonal = half == col
    flipped = (1 - half) * 2 + core
    x_peer = {"tau": tau, "row": row, "col": 1 - col}
    y_peer = {"tau": tau, "row": flipped, "col": col}
    far_peer = {"tau": tau, "row": flipped, "col": 1 - col}
    twin = {"tau": tau, "row": half * 2 + 1 - core, "col": col}
    steps = 2 * taus
    rows = ob.shape[2]
    depth = virt.shape[0]
    block = occ.shape[0] // om.shape[0]
    cols = virt.shape[1]
    near_only, far_only = 2, 3
    shared = steps - 2
    top, bottom = pl.ds(0, rows // 2), pl.ds(rows // 2, rows // 2)

    def start_row(step):
        return lax.rem(tau + 1 + step // 2, taus) * (2 * rows) + (step % 2) * rows

    def z_peer(step):
        return {"tau": lax.rem(tau + 1 + step // 2, taus), "row": row, "col": col}

    def remote(src, dst, send, recv, peer):
        return pltpu.make_async_remote_copy(
            src_ref=src, dst_ref=dst, send_sem=send, recv_sem=recv, device_id=peer, device_id_type=MESH
        )

    mine = pl.ds(pl.multiple_of(core * depth, depth), depth)
    v_local = pltpu.make_async_copy(virt, vbuf.at[mine, :], v_sem.at[0])
    v_local.start()

    barrier = pltpu.get_barrier_semaphore()
    peers = [x_peer, y_peer, far_peer, twin] + [z_peer(2 * s) for s in range(taus - 1)]
    for peer in peers:
        pl.semaphore_signal(barrier, inc=1, device_id=peer, device_id_type=MESH)
    pl.semaphore_wait(barrier, len(peers))

    def o_src(step):
        return occ.at[pl.ds(pl.multiple_of(start_row(step), rows), rows), :]

    def on_diagonal(step):
        return remote(o_src(step), ob.at[step, 1], o_send.at[step, 0], o_recv.at[step, 1], x_peer)

    def own(step):
        return pltpu.make_async_copy(o_src(step), ob.at[step, 1], o_recv.at[step, 1])

    def near(step):
        return remote(o_src(step), ob.at[step, 0], o_send.at[step, 0], o_recv.at[step, 0], y_peer)

    def far(step):
        return remote(o_src(step), ob.at[step, 0], o_send.at[step, 1], o_recv.at[step, 0], far_peer)

    def forward(step):
        return remote(ob.at[step, 0], ob.at[step, 0], f_send.at[0], o_recv.at[step, 0], x_peer)

    def half_src(side):
        at = start_row(shared) + side * (rows // 2)
        return occ.at[pl.ds(pl.multiple_of(at, rows // 2), rows // 2), :]

    def half_near():
        return remote(half_src(0), ob.at[shared, 0, top], o_send.at[shared, 0], h_recv.at[0], y_peer)

    def half_far():
        return remote(half_src(1), ob.at[shared, 0, bottom], o_send.at[shared, 1], h_recv.at[1], far_peer)

    def half_forward(side):
        part = ob.at[shared, 0, bottom if side else top]
        return remote(part, part, f_send.at[1], h_recv.at[side], x_peer)

    def half_arrived(side):
        return pltpu.make_async_copy(half_src(side), ob.at[shared, 0, bottom if side else top], h_recv.at[side])

    def arrived(step, slot):
        return pltpu.make_async_copy(o_src(step), ob.at[step, slot], o_recv.at[step, slot])

    m_x = remote(om, oraw.at[1], m_send.at[0], m_recv.at[1], x_peer)
    m_own = pltpu.make_async_copy(om, oraw.at[1], m_recv.at[1])
    m_near = remote(om, oraw.at[0], m_send.at[0], m_recv.at[0], y_peer)
    m_far = remote(om, oraw.at[0], m_send.at[1], m_recv.at[0], far_peer)
    v_remote = remote(virt, vbuf.at[mine, :], v_sem.at[1], v_sem.at[2], twin)
    vm_remote = remote(vm, vraw, v_sem.at[3], v_sem.at[4], twin)

    @pl.when(diagonal)
    def _():
        m_x.start()
        m_own.start()
        for step in range(4):
            on_diagonal(step).start()
            own(step).start()

    @pl.when(jnp.logical_not(diagonal))
    def _():
        m_far.start()
        m_near.start()
        far(0).start()
        near(0).start()
        far(far_only).start()
        near(near_only).start()
        far(1).start()
        near(1).start()
        half_far().start()
        half_near().start()
        for step in range(4, 6):
            far(step).start()
            near(step).start()

    vm_remote.start()
    v_remote.start()

    vm_rows = vm.shape[1]
    deep = depth // vm_rows

    def mask_virt(base):
        def one(b, _):
            r = pl.ds(pl.multiple_of((base + b) * deep, deep), deep)
            flags = vmask[pl.ds(base + b, 1), :]
            vbuf[r, :] = vbuf[r, :] * jnp.broadcast_to(flags, (deep, cols)).astype(vbuf.dtype)
            return 0

        lax.fori_loop(0, vm_rows, one, 0)

    width = cols // vm.shape[0]
    vmask[pl.ds(pl.multiple_of(core * vm_rows, vm_rows), vm_rows), :] = spread(vm[...], width, True)
    cmask[...] = spread(cm[...], cols // cm.shape[1])
    vm_remote.wait_recv()
    vmask[pl.ds(pl.multiple_of((1 - core) * vm_rows, vm_rows), vm_rows), :] = spread(vraw[...], width, True)
    v_local.wait()
    mask_virt(core * vm_rows)
    for slot in range(2):
        pltpu.make_async_copy(om, oraw.at[slot], m_recv.at[slot]).wait()
        omask[slot] = spread(oraw[slot], occ.shape[1] // om.shape[1])
    v_remote.wait_recv()
    mask_virt((1 - core) * vm_rows)

    tile = 256

    def partial_copy(step, side):
        part = pl.ds(side * (cols // 2), cols // 2)
        return remote(
            pbuf.at[step, :, part], rbuf.at[step, :, part], p_send.at[step, side], p_recv.at[step, side], y_peer
        )

    def z_copy(step):
        dst = zbuf.at[tau, pl.ds((step % 2) * rows, rows), :]
        return remote(cbuf.at[step], dst, z_send.at[step], z_recv.at[step], z_peer(step))

    def flag_row(step):
        return start_row(step) // block

    def finish(step):
        partial_copy(step, 0).wait_recv()
        partial_copy(step, 1).wait_recv()
        flags = jnp.broadcast_to(cmask[pl.ds(flag_row(step), 1), :], (rows, cols))
        chi = ((pa[step % 2] + rbuf[step].astype(jnp.float32)) * flags).astype(jnp.bfloat16)
        if step < steps - 2:
            cbuf[step] = chi
            z_copy(step).start()
        else:
            zbuf[tau, pl.ds((step % 2) * rows, rows), :] = chi

    def load(step, slot):
        def wait():
            arrived(step, slot).wait()

        if slot == 0 and step == near_only:
            pl.when(jnp.logical_not(diagonal))(wait)
        elif slot == 0 and step == far_only:
            pl.when(diagonal)(wait)
        elif slot == 0 and step == shared:
            pl.when(diagonal)(lambda: half_arrived(1).wait())
            pl.when(jnp.logical_not(diagonal))(lambda: half_arrived(0).wait())
        else:
            wait()
        flags = omask[slot, pl.ds(flag_row(step), 1), :]
        lhs[pl.ds(slot * rows, rows), :] = ob[step, slot] * jnp.broadcast_to(
            flags, (rows, lhs.shape[1])
        ).astype(lhs.dtype)

    for step in range(-1, steps):
        ahead = step + 1
        first, last = step < 0, ahead == steps
        if not last:
            load(ahead, 0)
        if not first:
            load(step, 1)

        def one(n, _, step=step, ahead=ahead, first=first, last=last):
            c = pl.ds(pl.multiple_of(n * tile, tile), tile)
            base, end = (rows if last else 0), (rows if first else 2 * rows)
            r = jnp.dot(lhs[base:end, :], vbuf[:, c], preferred_element_type=jnp.float32)
            if not last:
                pbuf[ahead, :, c] = r[:rows].astype(jnp.bfloat16)
            if not first:
                pa[step % 2, :, c] = r[rows - base :]
            return 0

        halves = cols // tile // 2
        lax.fori_loop(0, halves, one, 0)
        if not last:
            partial_copy(ahead, 0).start()
        lax.fori_loop(halves, 2 * halves, one, 0)
        if not last:
            partial_copy(ahead, 1).start()

        @pl.when(diagonal)
        def _(ahead=ahead, first=first):
            if first:
                arrived(near_only, 0).wait()
                forward(near_only).start()
            if ahead == 2:
                half_arrived(0).wait()
                half_forward(0).start()
            for later in (range(4, 6) if first else range(6, steps) if ahead == 2 else ()):
                if later < steps:
                    on_diagonal(later).start()
                    own(later).start()

        @pl.when(jnp.logical_not(diagonal))
        def _(ahead=ahead, first=first):
            if first:
                arrived(far_only, 0).wait()
                forward(far_only).start()
            if ahead == 2:
                half_arrived(1).wait()
                half_forward(1).start()
            if ahead + 6 < steps and ahead + 6 != shared:
                far(ahead + 6).start()
                near(ahead + 6).start()

        if not first:
            finish(step)

    for step in range(steps - 2):
        z_copy(step).wait_recv()
    for step in range(steps - 2):
        z_copy(step).wait_send()
    for step in range(steps):
        partial_copy(step, 0).wait_send()
        partial_copy(step, 1).wait_send()

    @pl.when(diagonal)
    def _():
        for step in range(steps):
            on_diagonal(step).wait_send()
        forward(near_only).wait_send()
        half_forward(0).wait_send()
        m_x.wait_send()

    @pl.when(jnp.logical_not(diagonal))
    def _():
        for step in range(steps):
            if step not in (near_only, shared):
                far(step).wait_send()
            if step not in (far_only, shared):
                near(step).wait_send()
        half_far().wait_send()
        half_near().wait_send()
        forward(far_only).wait_send()
        half_forward(1).wait_send()
        m_far.wait_send()
        m_near.wait_send()

    v_remote.wait_send()
    vm_remote.wait_send()


def transform(w, z, out):
    points = [z[t].astype(jnp.float32) for t in range(z.shape[0])]
    for k in range(out.shape[0]):
        total = w[k, 0] * points[0]
        for t in range(1, len(points)):
            total = total + w[k, t] * points[t]
        out[k] = total


def exchanged(taus, occupied, virtual_green, occ_mask, virt_mask, chi_mask, cosine_weights):
    occ, virt = occupied[0], virtual_green[0]
    m, k = occ.shape
    depth, cols = virt.shape
    rows = m // (2 * taus)
    steps = 2 * taus
    bf16, f32, i32 = jnp.bfloat16, jnp.float32, jnp.int32
    dma = pltpu.SemaphoreType.DMA
    vmem = pl.BlockSpec(memory_space=pltpu.VMEM)
    vm = virt_mask.T
    points = pl.pallas_call(
        functools.partial(kernel, taus),
        out_shape=jax.ShapeDtypeStruct((taus, 2 * rows, cols), bf16),
        in_specs=[pl.BlockSpec(memory_space=pl.ANY), pl.BlockSpec(memory_space=pl.ANY), vmem, vmem, vmem],
        out_specs=vmem,
        scratch_shapes=[
            pltpu.VMEM((2 * depth, cols), bf16),
            pltpu.VMEM(vm.shape, i32),
            pltpu.VMEM((2 * vm.shape[1], cols), f32),
            pltpu.VMEM((steps, 2, rows, k), bf16),
            pltpu.VMEM((2,) + occ_mask.shape, i32),
            pltpu.VMEM((2, occ_mask.shape[0], k), f32),
            pltpu.VMEM((chi_mask.shape[0], cols), f32),
            pltpu.VMEM((2 * rows, k), bf16),
            pltpu.VMEM((2, rows, cols), f32),
            pltpu.VMEM((steps, rows, cols), bf16),
            pltpu.VMEM((steps, rows, cols), bf16),
            pltpu.VMEM((steps, rows, cols), bf16),
            dma((5,)),
            dma((steps, 2)),
            dma((steps, 2)),
            dma((2,)),
            dma((2,)),
            dma((2,)),
            dma((2,)),
            dma((steps, 2)),
            dma((steps, 2)),
            dma((steps,)),
            dma((steps,)),
        ],
        compiler_params=pltpu.CompilerParams(collective_id=0, has_side_effects=True),
    )(occ, virt, occ_mask, vm, chi_mask)
    freqs = cosine_weights.shape[0]
    return pl.pallas_call(
        transform,
        grid=(2,),
        out_shape=jax.ShapeDtypeStruct((freqs, 2 * rows, cols), f32),
        in_specs=[
            pl.BlockSpec(memory_space=pltpu.SMEM),
            pl.BlockSpec((taus, rows, cols), lambda i: (0, i, 0)),
        ],
        out_specs=pl.BlockSpec((freqs, rows, cols), lambda i: (0, i, 0)),
    )(cosine_weights, points)


def solution(mesh):
    placed = (
        P("tau", "row", "col"),
        P("tau", "row", "col"),
        P("row", "col"),
        P("row", "col"),
        P("row", "col"),
        P(),
    )
    plane = mesh.shape["row"] == 4 and mesh.shape["col"] == 2 and mesh.shape["tau"] > 3
    return jax.shard_map(
        functools.partial(exchanged, mesh.shape["tau"]) if plane else gathered,
        mesh=mesh,
        in_specs=placed,
        out_specs=P(None, ("row", "tau"), "col"),
        check_vma=False,
    )
```

```python
import functools

import jax
import jax.numpy as jnp
from jax import lax
from jax.experimental import pallas as pl
from jax.experimental.pallas import tpu as pltpu
from jax.sharding import PartitionSpec as P

MESH = pl.DeviceIdType.MESH


def expand_mask(values, flags):
    block_rows = values.shape[0] // flags.shape[0]
    block_cols = values.shape[1] // flags.shape[1]
    shaped = values.reshape(flags.shape[0], block_rows, flags.shape[1], block_cols)
    masked = shaped * flags.astype(values.dtype)[:, None, :, None]
    return masked.reshape(values.shape)


def gathered(occupied, virtual_green, occ_mask, virt_mask, chi_mask, cosine_weights):
    occ_tile = expand_mask(occupied[0], occ_mask)
    virt_tile = expand_mask(virtual_green[0], virt_mask)
    virt_column = lax.all_gather(virt_tile, "row", axis=0, tiled=True)
    accumulated = jnp.dot(
        lax.all_gather(occ_tile, "col", axis=1, tiled=True),
        virt_column,
        preferred_element_type=jnp.float32,
    )
    chi_local = expand_mask(accumulated, chi_mask).astype(jnp.bfloat16)
    regrouped = lax.all_to_all(chi_local[None], "tau", split_axis=1, concat_axis=0, tiled=True)
    return jnp.einsum(
        "kt,tij->kij",
        cosine_weights,
        regrouped.astype(jnp.float32),
        precision=lax.Precision.HIGHEST,
    )


def spread(flags, width, transposed=False):
    dim = 0 if transposed else 1
    count = flags.shape[dim]
    owner = lax.broadcasted_iota(jnp.int32, (count, count * width), 1) // width
    mine = owner == lax.broadcasted_iota(jnp.int32, (count, count * width), 0)
    return lax.dot_general(
        flags.astype(jnp.float32),
        mine.astype(jnp.float32),
        (((dim,), (0,)), ((), ())),
        preferred_element_type=jnp.float32,
    )


def kernel(
    taus, occ, virt, om, vm, cm, zbuf,
    vbuf, vraw, vmask, ob, oraw, omask, cmask, lhs, pa, pbuf, rbuf, cbuf,
    v_sem, o_send, o_recv, h_recv, f_send, m_send, m_recv, p_send, p_recv, z_send, z_recv,
):
    tau, row, col = lax.axis_index("tau"), lax.axis_index("row"), lax.axis_index("col")
    half, core = row // 2, row % 2
    diagonal = half == col
    flipped = (1 - half) * 2 + core
    x_peer = {"tau": tau, "row": row, "col": 1 - col}
    y_peer = {"tau": tau, "row": flipped, "col": col}
    far_peer = {"tau": tau, "row": flipped, "col": 1 - col}
    twin = {"tau": tau, "row": half * 2 + 1 - core, "col": col}
    steps = 2 * taus
    rows = ob.shape[2]
    depth = virt.shape[0]
    block = occ.shape[0] // om.shape[0]
    cols = virt.shape[1]
    near_only, far_only = 3, 2
    shared = steps - 2
    top, bottom = pl.ds(0, rows // 2), pl.ds(rows // 2, rows // 2)

    def start_row(step):
        return lax.rem(tau + 1 + step // 2, taus) * (2 * rows) + (step % 2) * rows

    def z_peer(step):
        return {"tau": lax.rem(tau + 1 + step // 2, taus), "row": row, "col": col}

    def remote(src, dst, send, recv, peer):
        return pltpu.make_async_remote_copy(
            src_ref=src, dst_ref=dst, send_sem=send, recv_sem=recv, device_id=peer, device_id_type=MESH
        )

    mine = pl.ds(pl.multiple_of(core * depth, depth), depth)
    v_local = pltpu.make_async_copy(virt, vbuf.at[mine, :], v_sem.at[0])
    v_local.start()

    barrier = pltpu.get_barrier_semaphore()
    peers = [x_peer, y_peer, far_peer, twin] + [z_peer(2 * s) for s in range(taus - 1)]
    for peer in peers:
        pl.semaphore_signal(barrier, inc=1, device_id=peer, device_id_type=MESH)
    pl.semaphore_wait(barrier, len(peers))

    def o_src(step):
        return occ.at[pl.ds(pl.multiple_of(start_row(step), rows), rows), :]

    def on_diagonal(step):
        return remote(o_src(step), ob.at[step, 1], o_send.at[step, 0], o_recv.at[step, 1], x_peer)

    def own(step):
        return pltpu.make_async_copy(o_src(step), ob.at[step, 1], o_recv.at[step, 1])

    def near(step):
        return remote(o_src(step), ob.at[step, 0], o_send.at[step, 0], o_recv.at[step, 0], y_peer)

    def far(step):
        return remote(o_src(step), ob.at[step, 0], o_send.at[step, 1], o_recv.at[step, 0], far_peer)

    def forward(step):
        return remote(ob.at[step, 0], ob.at[step, 0], f_send.at[0], o_recv.at[step, 0], x_peer)

    def half_src(side):
        at = start_row(shared) + side * (rows // 2)
        return occ.at[pl.ds(pl.multiple_of(at, rows // 2), rows // 2), :]

    def half_near():
        return remote(half_src(0), ob.at[shared, 0, top], o_send.at[shared, 0], h_recv.at[0], y_peer)

    def half_far():
        return remote(half_src(1), ob.at[shared, 0, bottom], o_send.at[shared, 1], h_recv.at[1], far_peer)

    def half_forward(side):
        part = ob.at[shared, 0, bottom if side else top]
        return remote(part, part, f_send.at[1], h_recv.at[side], x_peer)

    def half_arrived(side):
        return pltpu.make_async_copy(half_src(side), ob.at[shared, 0, bottom if side else top], h_recv.at[side])

    def arrived(step, slot):
        return pltpu.make_async_copy(o_src(step), ob.at[step, slot], o_recv.at[step, slot])

    m_x = remote(om, oraw.at[1], m_send.at[0], m_recv.at[1], x_peer)
    m_own = pltpu.make_async_copy(om, oraw.at[1], m_recv.at[1])
    m_near = remote(om, oraw.at[0], m_send.at[0], m_recv.at[0], y_peer)
    m_far = remote(om, oraw.at[0], m_send.at[1], m_recv.at[0], far_peer)
    v_remote = remote(virt, vbuf.at[mine, :], v_sem.at[1], v_sem.at[2], twin)
    vm_remote = remote(vm, vraw, v_sem.at[3], v_sem.at[4], twin)

    @pl.when(diagonal)
    def _():
        m_x.start()
        m_own.start()
        for step in range(4):
            on_diagonal(step).start()
            own(step).start()

    @pl.when(jnp.logical_not(diagonal))
    def _():
        m_far.start()
        m_near.start()
        far(0).start()
        near(0).start()
        far(far_only).start()
        near(near_only).start()
        far(1).start()
        near(1).start()
        half_far().start()
        half_near().start()
        for step in range(4, 5):
            far(step).start()
            near(step).start()

    vm_remote.start()
    v_remote.start()

    vm_rows = vm.shape[1]
    deep = depth // vm_rows

    def mask_virt(base):
        def one(b, _):
            r = pl.ds(pl.multiple_of((base + b) * deep, deep), deep)
            flags = vmask[pl.ds(base + b, 1), :]
            vbuf[r, :] = vbuf[r, :] * jnp.broadcast_to(flags, (deep, cols)).astype(vbuf.dtype)
            return 0

        lax.fori_loop(0, vm_rows, one, 0)

    width = cols // vm.shape[0]
    vmask[pl.ds(pl.multiple_of(core * vm_rows, vm_rows), vm_rows), :] = spread(vm[...], width, True)
    cmask[...] = spread(cm[...], cols // cm.shape[1])
    vm_remote.wait_recv()
    vmask[pl.ds(pl.multiple_of((1 - core) * vm_rows, vm_rows), vm_rows), :] = spread(vraw[...], width, True)
    v_local.wait()
    mask_virt(core * vm_rows)
    for slot in range(2):
        pltpu.make_async_copy(om, oraw.at[slot], m_recv.at[slot]).wait()
        omask[slot] = spread(oraw[slot], occ.shape[1] // om.shape[1])
    v_remote.wait_recv()
    mask_virt((1 - core) * vm_rows)

    tile = 256

    def partial_copy(step, side):
        part = pl.ds(side * (cols // 2), cols // 2)
        return remote(
            pbuf.at[step, :, part], rbuf.at[step, :, part], p_send.at[step, side], p_recv.at[step, side], y_peer
        )

    def z_copy(step):
        dst = zbuf.at[tau, pl.ds((step % 2) * rows, rows), :]
        return remote(cbuf.at[step], dst, z_send.at[step], z_recv.at[step], z_peer(step))

    def flag_row(step):
        return start_row(step) // block

    def finish(step):
        partial_copy(step, 0).wait_recv()
        partial_copy(step, 1).wait_recv()
        flags = jnp.broadcast_to(cmask[pl.ds(flag_row(step), 1), :], (rows, cols))
        chi = ((pa[step % 2] + rbuf[step].astype(jnp.float32)) * flags).astype(jnp.bfloat16)
        if step < steps - 2:
            cbuf[step] = chi
            z_copy(step).start()
        else:
            zbuf[tau, pl.ds((step % 2) * rows, rows), :] = chi

    def load(step, slot):
        def wait():
            arrived(step, slot).wait()

        if slot == 0 and step == near_only:
            pl.when(jnp.logical_not(diagonal))(wait)
        elif slot == 0 and step == far_only:
            pl.when(diagonal)(wait)
        elif slot == 0 and step == shared:
            pl.when(diagonal)(lambda: half_arrived(1).wait())
            pl.when(jnp.logical_not(diagonal))(lambda: half_arrived(0).wait())
        else:
            wait()
        flags = omask[slot, pl.ds(flag_row(step), 1), :]
        lhs[pl.ds(slot * rows, rows), :] = ob[step, slot] * jnp.broadcast_to(
            flags, (rows, lhs.shape[1])
        ).astype(lhs.dtype)

    for step in range(-1, steps):
        ahead = step + 1
        first, last = step < 0, ahead == steps
        if not last:
            load(ahead, 0)
        if not first:
            load(step, 1)

        def one(n, _, step=step, ahead=ahead, first=first, last=last):
            c = pl.ds(pl.multiple_of(n * tile, tile), tile)
            base, end = (rows if last else 0), (rows if first else 2 * rows)
            r = jnp.dot(lhs[base:end, :], vbuf[:, c], preferred_element_type=jnp.float32)
            if not last:
                pbuf[ahead, :, c] = r[:rows].astype(jnp.bfloat16)
            if not first:
                pa[step % 2, :, c] = r[rows - base :]
            return 0

        halves = cols // tile // 2
        lax.fori_loop(0, halves, one, 0)
        if not last:
            partial_copy(ahead, 0).start()
        lax.fori_loop(halves, 2 * halves, one, 0)
        if not last:
            partial_copy(ahead, 1).start()

        @pl.when(diagonal)
        def _(ahead=ahead, first=first):
            if first:
                arrived(near_only, 0).wait()
                forward(near_only).start()
            if ahead == 2:
                half_arrived(0).wait()
                half_forward(0).start()
            for later in (range(4, 6) if first else range(6, steps) if ahead == 2 else ()):
                if later < steps:
                    on_diagonal(later).start()
                    own(later).start()

        @pl.when(jnp.logical_not(diagonal))
        def _(ahead=ahead, first=first):
            if first:
                arrived(far_only, 0).wait()
                forward(far_only).start()
            if ahead == 2:
                half_arrived(1).wait()
                half_forward(1).start()
            if ahead + 5 < steps and ahead + 5 != shared:
                far(ahead + 5).start()
                near(ahead + 5).start()

        if not first:
            finish(step)

    for step in range(steps - 2):
        z_copy(step).wait_recv()
    for step in range(steps - 2):
        z_copy(step).wait_send()
    for step in range(steps):
        partial_copy(step, 0).wait_send()
        partial_copy(step, 1).wait_send()

    @pl.when(diagonal)
    def _():
        for step in range(steps):
            on_diagonal(step).wait_send()
        forward(near_only).wait_send()
        half_forward(0).wait_send()
        m_x.wait_send()

    @pl.when(jnp.logical_not(diagonal))
    def _():
        for step in range(steps):
            if step not in (near_only, shared):
                far(step).wait_send()
            if step not in (far_only, shared):
                near(step).wait_send()
        half_far().wait_send()
        half_near().wait_send()
        forward(far_only).wait_send()
        half_forward(1).wait_send()
        m_far.wait_send()
        m_near.wait_send()

    v_remote.wait_send()
    vm_remote.wait_send()


def transform(w, z, out):
    points = [z[t].astype(jnp.float32) for t in range(z.shape[0])]
    for k in range(out.shape[0]):
        total = w[k, 0] * points[0]
        for t in range(1, len(points)):
            total = total + w[k, t] * points[t]
        out[k] = total


def exchanged(taus, occupied, virtual_green, occ_mask, virt_mask, chi_mask, cosine_weights):
    occ, virt = occupied[0], virtual_green[0]
    m, k = occ.shape
    depth, cols = virt.shape
    rows = m // (2 * taus)
    steps = 2 * taus
    bf16, f32, i32 = jnp.bfloat16, jnp.float32, jnp.int32
    dma = pltpu.SemaphoreType.DMA
    vmem = pl.BlockSpec(memory_space=pltpu.VMEM)
    vm = virt_mask.T
    points = pl.pallas_call(
        functools.partial(kernel, taus),
        out_shape=pltpu.VMEM((taus, 2 * rows, cols), bf16),
        in_specs=[pl.BlockSpec(memory_space=pl.ANY), pl.BlockSpec(memory_space=pl.ANY), vmem, vmem, vmem],
        out_specs=vmem,
        scratch_shapes=[
            pltpu.VMEM((2 * depth, cols), bf16),
            pltpu.VMEM(vm.shape, i32),
            pltpu.VMEM((2 * vm.shape[1], cols), f32),
            pltpu.VMEM((steps, 2, rows, k), bf16),
            pltpu.VMEM((2,) + occ_mask.shape, i32),
            pltpu.VMEM((2, occ_mask.shape[0], k), f32),
            pltpu.VMEM((chi_mask.shape[0], cols), f32),
            pltpu.VMEM((2 * rows, k), bf16),
            pltpu.VMEM((2, rows, cols), f32),
            pltpu.VMEM((steps, rows, cols), bf16),
            pltpu.VMEM((steps, rows, cols), bf16),
            pltpu.VMEM((steps, rows, cols), bf16),
            dma((5,)),
            dma((steps, 2)),
            dma((steps, 2)),
            dma((2,)),
            dma((2,)),
            dma((2,)),
            dma((2,)),
            dma((steps, 2)),
            dma((steps, 2)),
            dma((steps,)),
            dma((steps,)),
        ],
        compiler_params=pltpu.CompilerParams(collective_id=0, has_side_effects=True),
    )(occ, virt, occ_mask, vm, chi_mask)
    freqs = cosine_weights.shape[0]
    return pl.pallas_call(
        transform,
        grid=(2,),
        out_shape=jax.ShapeDtypeStruct((freqs, 2 * rows, cols), f32),
        in_specs=[
            pl.BlockSpec(memory_space=pltpu.SMEM),
            pl.BlockSpec((taus, rows, cols), lambda i: (0, i, 0)),
        ],
        out_specs=pl.BlockSpec((freqs, rows, cols), lambda i: (0, i, 0)),
    )(cosine_weights, points)


def solution(mesh):
    placed = (
        P("tau", "row", "col"),
        P("tau", "row", "col"),
        P("row", "col"),
        P("row", "col"),
        P("row", "col"),
        P(),
    )
    plane = mesh.shape["row"] == 4 and mesh.shape["col"] == 2 and mesh.shape["tau"] > 3
    return jax.shard_map(
        functools.partial(exchanged, mesh.shape["tau"]) if plane else gathered,
        mesh=mesh,
        in_specs=placed,
        out_specs=P(None, ("row", "tau"), "col"),
        check_vma=False,
    )
```
